32 devices in a mesh: trial: 4 (over y, x), rows: 2 (over core), cols: 4 (over z).
Axes of the slice: x: 2, y: 2, z: 4, core: 2. Of those that a mesh axis runs over, the one named last changes fastest.
Arguments:
- weight_gate: float32 [8192, 8192], P(('trial', 'rows'), 'cols'), parts along dimension 0, may hold values from -0.1875 to 0.1875
- moment_gate: float32 [8192, 8192], P(('trial', 'rows'), 'cols'), parts along dimension 0, may hold values from -6 to 6
- square_gate: float32 [8192, 8192], P(('trial', 'rows'), 'cols'), parts along dimension 0, may hold values from 0.1 to 10
- weight_up: float32 [8192, 8192], P(('trial', 'rows'), 'cols'), parts along dimension 0, may hold values from -0.1875 to 0.1875
- moment_up: float32 [8192, 8192], P(('trial', 'rows'), 'cols'), parts along dimension 0, may hold values from -6 to 6
- square_up: float32 [8192, 8192], P(('trial', 'rows'), 'cols'), parts along dimension 0, may hold values from 0.1 to 10
- norm_gain: float32 [8192], P(('trial', 'rows')), parts along dimension 0, may hold values from 0.25 to 1.75
Outputs:
- serving_gate: bfloat16 [8192, 8192], P('trial', 'cols'), parts along dimension 0
- serving_up: bfloat16 [8192, 8192], P('trial', 'cols'), parts along dimension 0
- column_gate: float32 [32768], P(('trial', 'cols')), parts along dimension 0
- column_up: float32 [32768], P(('trial', 'cols')), parts along dimension 0
The draws below stay inside these ranges and needn't reach their ends.
There are 4 independent parts, one for each index of `trial`. The reference program is written for one: setup_inputs(seed, part) draws one part's arguments, and reference() takes and returns one part's arrays. A program takes and returns all parts, laid end to end along the dimension named above; each array names one. Nothing has to cross between parts.
All inputs are finite; a program needn't handle non-finite values. Where the reference program divides by a largest or mean magnitude, that divisor is 1e-20 or more.
Results may differ from the reference program's by a relative error of at most 0.001.
Values may be sent and summed in bfloat16 or wider, within the bound.
A program may use at most 128 MiB of HBM per device.

```python
import math
import jax
import jax.numpy as jnp
from jax import lax

D_MODEL = 2048
D_INNER = 8192


def strengthened(array, stream_key, source, target, blocks, factor):
    def block_of(dim):
        return (jnp.arange(array.shape[dim]) // (array.shape[dim] // blocks)).reshape((-1,) + (1,) * (array.ndim - 1 - dim))

    first = jax.random.permutation(stream_key, blocks)[block_of(target)]
    far = (block_of(target) + blocks // 2) % blocks
    return jnp.where((block_of(source) == first) | (block_of(source) == far), factor * array, array)


def shard_levels(stream_key, extent, cuts, least, high):
    def one(axis_at, shards_of):
        draws = jax.random.uniform(jax.random.fold_in(jax.random.fold_in(stream_key, 6), axis_at), (shards_of,), jnp.float32, least / len(cuts), high / len(cuts))
        return jnp.repeat(jnp.exp(draws), extent[axis_at] // shards_of).reshape((-1,) + (1,) * (len(extent) - axis_at - 1))

    level = one(*cuts[0])
    for cut in cuts[1:]:
        level = level * one(*cut)
    return level


def gaussian(own_key, extent, width, bound, split=(), held_as=jnp.bfloat16):
    drawn = jax.random.normal(own_key, extent, jnp.float32) * width
    if len(split) > 0:
        drawn = shard_levels(own_key, extent, split, -0.22, 0.18) * drawn
    return jnp.clip(drawn, min=-bound, max=bound).astype(held_as)


def bell_draw_with(key, extent, width, bound, shards, heavy, kind=jnp.bfloat16):
    values = width * jax.random.normal(key, extent, jnp.float32)
    if shards:
        values = values * shard_levels(key, extent, shards, -0.22, 0.18)
    return jnp.clip(strengthened(values, jax.random.fold_in(key, 3), *heavy), -bound, bound).astype(kind)


def setup_inputs(seed: int = 0, part: int = 0) -> dict:
    splits = jax.random.split(jax.random.key(seed), 8)
    own_keys = jax.random.split(jax.random.fold_in(splits[7], part), 8)
    return {
        "weight_gate": bell_draw_with(own_keys[0], (D_MODEL, D_INNER), D_MODEL ** -0.5, 0.1875, ((0, 2), (1, 4)), (0, 1, 4, 2.0), jnp.float32),
        "moment_gate": gaussian(own_keys[1], (D_MODEL, D_INNER), 1.0, 6.0, ((0, 2), (1, 4)), jnp.float32),
        "square_gate": jnp.clip(jnp.exp(math.log(10.0) - 4.6051702 * jax.random.uniform(own_keys[2], (D_MODEL, D_INNER), jnp.float32) ** shard_levels(own_keys[2], (D_MODEL, D_INNER), ((0, 2), (1, 4)), -0.2, 0.2)), 0.1, 10.0),
        "weight_up": bell_draw_with(own_keys[3], (D_MODEL, D_INNER), D_MODEL ** -0.5, 0.1875, ((0, 2), (1, 4)), (0, 1, 4, 2.0), jnp.float32),
        "moment_up": gaussian(own_keys[4], (D_MODEL, D_INNER), 1.0, 6.0, ((0, 2), (1, 4)), jnp.float32),
        "square_up": jnp.clip(jnp.exp(math.log(10.0) - 4.6051702 * jax.random.uniform(own_keys[5], (D_MODEL, D_INNER), jnp.float32) ** shard_levels(own_keys[5], (D_MODEL, D_INNER), ((0, 2), (1, 4)), -0.2, 0.2)), 0.1, 10.0),
        "norm_gain": jnp.clip(1.0 + 0.15 * jax.random.normal(own_keys[6], (D_MODEL,), jnp.float32), 0.25, 1.75),
    }


learn_rate = 0.02
decay_rate = 0.05
tiny_value = 1e-08

def reference(weight_gate, moment_gate, square_gate, weight_up, moment_up, square_up, norm_gain):
    whole_gate = weight_gate - learn_rate * (moment_gate / (jnp.sqrt(square_gate) + tiny_value) + decay_rate * weight_gate)
    whole_up = weight_up - learn_rate * (moment_up / (jnp.sqrt(square_up) + tiny_value) + decay_rate * weight_up)
    whole_gained_gate = whole_gate * norm_gain[:, None]
    whole_gained_up = whole_up * norm_gain[:, None]
    column_gate = lax.optimization_barrier(jnp.sum(jnp.abs(whole_gained_gate), axis=0)) / D_MODEL
    serving_gate = (whole_gained_gate / column_gate).astype(jnp.bfloat16)
    column_up = lax.optimization_barrier(jnp.sum(jnp.abs(whole_gained_up), axis=0)) / D_MODEL
    serving_up = (whole_gained_up / column_up).astype(jnp.bfloat16)
    return (serving_gate, serving_up, column_gate, column_up)
```

```python
import functools

import jax
import jax.numpy as jnp
from jax import lax
from jax.experimental import pallas as pl
from jax.experimental.pallas import tpu as pltpu
from jax.sharding import PartitionSpec as P

learn_rate = 0.02
decay_rate = 0.05
tiny_value = 1e-08

LANES = 128
SLAB = 256
SLOTS = 8
MESH = pl.DeviceIdType.MESH


def exchange_kernel(
    n, wg, mg, sg, wu, mu, su, gain, out_g, out_u, col_g, col_u,
    w_buf, m_buf, s_buf, held, keep_scale, step_scale, parts,
    in_sem, part_send, part_recv, row_send, row_recv,
):
    rows, width = wg.shape
    slabs = width // SLAB
    steps = 2 * slabs
    chunk = min(rows, 256)
    me = lax.axis_index("rows")
    sources = ((wg, mg, sg), (wu, mu, su))
    outs = (out_g, out_u)
    cols = (col_g, col_u)
    buffers = (w_buf, m_buf, s_buf)

    def columns(j):
        return pl.ds(pl.multiple_of(j * SLAB, SLAB), SLAB)

    def loads(j, p):
        slot = lax.rem(2 * j + p, SLOTS)
        return [
            pltpu.make_async_copy(source.at[:, columns(j)], buffer.at[slot], in_sem.at[slot, i])
            for i, (source, buffer) in enumerate(zip(sources[p], buffers))
        ]

    def part_copy(j, p, k, owner):
        t = 2 * j + p
        return pltpu.make_async_remote_copy(
            src_ref=parts.at[t, owner],
            dst_ref=parts.at[t, owner],
            send_sem=part_send.at[t, k - 1],
            recv_sem=part_recv.at[t, k - 1],
            device_id={"rows": lax.rem(me + k, n)},
            device_id_type=MESH,
        )

    def row_copy(j, p, k, owner):
        t = 2 * j + p
        block = outs[p].at[pl.ds(pl.multiple_of(owner * rows, rows), rows), columns(j)]
        return pltpu.make_async_remote_copy(
            src_ref=block,
            dst_ref=block,
            send_sem=row_send.at[t, k - 1],
            recv_sem=row_recv.at[t, k - 1],
            device_id={"rows": lax.rem(me + k, n)},
            device_id_type=MESH,
        )

    def update(j, p):
        slot = lax.rem(2 * j + p, SLOTS)
        for copy in loads(j, p):
            copy.wait()

        def body(c, sums):
            at = pl.ds(pl.multiple_of(c * chunk, chunk), chunk)
            keep, scale = keep_scale[at, :], step_scale[at, :]
            new = []
            for i in range(SLAB // LANES):
                tile = pl.ds(i * LANES, LANES)
                square = s_buf[slot, at, tile]
                root = square * lax.rsqrt(square)
                value = w_buf[slot, at, tile] * keep - (m_buf[slot, at, tile] * scale) / (root + tiny_value)
                held[p, at, tile] = value
                new.append(sums[i] + jnp.sum(jnp.abs(value).reshape(chunk // 8, 8, LANES), axis=0))
            return tuple(new)

        zero = jnp.zeros((8, LANES), jnp.float32)
        sums = lax.fori_loop(0, rows // chunk, body, (zero,) * (SLAB // LANES))
        for i in range(SLAB // LANES):
            parts[2 * j + p, me, :, pl.ds(i * LANES, LANES)] = sums[i]

    def share_sums(j, p):
        for k in range(1, n):
            part_copy(j, p, k, me).start()

    def finish(j, p):
        t = 2 * j + p
        for k in range(1, n):
            part_copy(j, p, k, lax.rem(me + n - k, n)).wait_recv()
        total = parts[t, 0]
        for r in range(1, n):
            total = total + parts[t, r]
        column = jnp.sum(total, axis=0, keepdims=True) / (n * rows)
        cols[p][:, columns(j)] = column
        factor = 1.0 / column

        def body(c, carry):
            at = pl.ds(pl.multiple_of(c * chunk, chunk), chunk)
            to = pl.ds(pl.multiple_of(me * rows + c * chunk, chunk), chunk)
            outs[p][to, columns(j)] = (held[p, at, :] * factor).astype(jnp.bfloat16)
            return carry

        lax.fori_loop(0, rows // chunk, body, 0)

    def share_rows(j, p):
        for k in range(1, n):
            row_copy(j, p, k, me).start()

    ahead = min(SLOTS // 2, slabs)
    for j in range(ahead):
        for p in range(2):
            for copy in loads(j, p):
                copy.start()

    barrier = pltpu.get_barrier_semaphore()
    for k in range(1, n):
        pl.semaphore_signal(barrier, inc=1, device_id={"rows": lax.rem(me + k, n)}, device_id_type=MESH)

    for r in range(rows // LANES):
        spread = jnp.broadcast_to(gain[r : r + 1, :], (LANES, LANES)).T
        at = pl.ds(r * LANES, LANES)
        keep_scale[at, :] = spread * (1.0 - learn_rate * decay_rate)
        step_scale[at, :] = spread * learn_rate

    pl.semaphore_wait(barrier, n - 1)

    def refill(j, p):
        @pl.when(j + ahead < slabs)
        def _():
            for copy in loads(j + ahead, p):
                copy.start()

    def step(j, carry):
        update(j, 0)
        share_sums(j, 0)
        refill(j, 0)

        @pl.when(j > 0)
        def _():
            finish(j - 1, 1)
            share_rows(j - 1, 1)

        update(j, 1)
        share_sums(j, 1)
        refill(j, 1)
        finish(j, 0)
        share_rows(j, 0)
        return carry

    lax.fori_loop(0, slabs, step, 0)
    finish(slabs - 1, 1)
    share_rows(slabs - 1, 1)

    def drain(j, carry):
        for p in range(2):
            for k in range(1, n):
                part_copy(j, p, k, me).wait_send()
                row_copy(j, p, k, me).wait_send()
                row_copy(j, p, k, lax.rem(me + n - k, n)).wait_recv()
        return carry

    lax.fori_loop(0, slabs, drain, 0)


def store_kernel(pieces, gate, up, col_g, col_u, out_g, out_u, out_cg, out_cu, sem, col_sem):
    height = gate.shape[0] // pieces
    copies = []
    for p, (source, target) in enumerate(((gate, out_g), (up, out_u))):
        for i in range(pieces):
            at = pl.ds(i * height, height)
            copies.append(pltpu.make_async_copy(source.at[at, :], target.at[at, :], sem.at[p, i]))
    copies.append(pltpu.make_async_copy(col_g, out_cg, col_sem.at[0]))
    copies.append(pltpu.make_async_copy(col_u, out_cu, col_sem.at[1]))
    for copy in copies:
        copy.start()
    for copy in copies:
        copy.wait()


def solution(mesh):
    n = mesh.shape["rows"]

    def shards(weight_gate, moment_gate, square_gate, weight_up, moment_up, square_up, norm_gain):
        rows, width = weight_gate.shape
        steps = 2 * (width // SLAB)
        any_space = pl.BlockSpec(memory_space=pl.ANY)
        in_vmem = pl.BlockSpec(memory_space=pltpu.VMEM)
        shapes = (
            ((n * rows, width), jnp.bfloat16),
            ((n * rows, width), jnp.bfloat16),
            ((1, width), jnp.float32),
            ((1, width), jnp.float32),
        )
        dma = pltpu.SemaphoreType.DMA
        moved = pl.pallas_call(
            functools.partial(exchange_kernel, n),
            out_shape=tuple(pltpu.VMEM(*shape) for shape in shapes),
            in_specs=[any_space] * 6 + [in_vmem],
            out_specs=[in_vmem] * 4,
            scratch_shapes=[
                pltpu.VMEM((SLOTS, rows, SLAB), jnp.float32),
                pltpu.VMEM((SLOTS, rows, SLAB), jnp.float32),
                pltpu.VMEM((SLOTS, rows, SLAB), jnp.float32),
                pltpu.VMEM((2, rows, SLAB), jnp.float32),
                pltpu.VMEM((rows, LANES), jnp.float32),
                pltpu.VMEM((rows, LANES), jnp.float32),
                pltpu.VMEM((steps, n, 8, SLAB), jnp.float32),
                dma((SLOTS, 3)),
                dma((steps, max(n - 1, 1))),
                dma((steps, max(n - 1, 1))),
                dma((steps, max(n - 1, 1))),
                dma((steps, max(n - 1, 1))),
            ],
            compiler_params=pltpu.CompilerParams(
                collective_id=0, has_side_effects=True, vmem_limit_bytes=36 * 1024 * 1024
            ),
            name="exchange",
        )(
            weight_gate, moment_gate, square_gate, weight_up, moment_up, square_up,
            norm_gain.reshape(rows // LANES, LANES),
        )
        pieces = 4
        gate, up, col_g, col_u = pl.pallas_call(
            functools.partial(store_kernel, pieces),
            out_shape=tuple(jax.ShapeDtypeStruct(*shape) for shape in shapes),
            in_specs=[in_vmem] * 4,
            out_specs=[any_space] * 4,
            scratch_shapes=[dma((2, pieces)), dma((2,))],
            compiler_params=pltpu.CompilerParams(vmem_limit_bytes=1024 * 1024),
            name="store",
        )(*moved)
        return gate, up, col_g.reshape(width), col_u.reshape(width)

    held = P(("trial", "rows"), "cols")
    return jax.shard_map(
        shards,
        mesh=mesh,
        in_specs=(held,) * 6 + (P(("trial", "rows")),),
        out_specs=(P("trial", "cols"), P("trial", "cols"), P(("trial", "cols")), P(("trial", "cols"))),
        check_vma=False,
    )
```

```python
import functools

import jax
import jax.numpy as jnp
from jax import lax
from jax.experimental import pallas as pl
from jax.experimental.pallas import tpu as pltpu
from jax.sharding import PartitionSpec as P

learn_rate = 0.02
decay_rate = 0.05
tiny_value = 1e-08

LANES = 128
SLAB = 256
SLOTS = 8
MESH = pl.DeviceIdType.MESH


def exchange_kernel(
    n, wg, mg, sg, wu, mu, su, gain, out_g, out_u, col_g, col_u,
    w_buf, m_buf, s_buf, held, gain_buf, keep_scale, step_scale, parts,
    gain_sem, in_sem, part_send, part_recv, row_send, row_recv,
):
    rows, width = wg.shape
    slabs = width // SLAB
    steps = 2 * slabs
    chunk = min(rows, 256)
    me = lax.axis_index("rows")
    sources = ((wg, mg, sg), (wu, mu, su))
    outs = (out_g, out_u)
    cols = (col_g, col_u)
    buffers = (w_buf, m_buf, s_buf)

    def columns(j):
        return pl.ds(pl.multiple_of(j * SLAB, SLAB), SLAB)

    def loads(j, p):
        slot = lax.rem(2 * j + p, SLOTS)
        return [
            pltpu.make_async_copy(source.at[:, columns(j)], buffer.at[slot], in_sem.at[slot, i])
            for i, (source, buffer) in enumerate(zip(sources[p], buffers))
        ]

    def part_copy(j, p, k, owner):
        t = 2 * j + p
        return pltpu.make_async_remote_copy(
            src_ref=parts.at[t, owner],
            dst_ref=parts.at[t, owner],
            send_sem=part_send.at[t, k - 1],
            recv_sem=part_recv.at[t, k - 1],
            device_id={"rows": lax.rem(me + k, n)},
            device_id_type=MESH,
        )

    def row_copy(j, p, k, owner):
        t = 2 * j + p
        block = outs[p].at[pl.ds(pl.multiple_of(owner * rows, rows), rows), columns(j)]
        return pltpu.make_async_remote_copy(
            src_ref=block,
            dst_ref=block,
            send_sem=row_send.at[t, k - 1],
            recv_sem=row_recv.at[t, k - 1],
            device_id={"rows": lax.rem(me + k, n)},
            device_id_type=MESH,
        )

    def update(j, p):
        slot = lax.rem(2 * j + p, SLOTS)
        for copy in loads(j, p):
            copy.wait()

        def body(c, sums):
            at = pl.ds(pl.multiple_of(c * chunk, chunk), chunk)
            keep, scale = keep_scale[at, :], step_scale[at, :]
            new = []
            for i in range(SLAB // LANES):
                tile = pl.ds(i * LANES, LANES)
                square = s_buf[slot, at, tile]
                root = square * lax.rsqrt(square)
                value = w_buf[slot, at, tile] * keep - (m_buf[slot, at, tile] * scale) / (root + tiny_value)
                held[p, at, tile] = value
                new.append(sums[i] + jnp.sum(jnp.abs(value).reshape(chunk // 8, 8, LANES), axis=0))
            return tuple(new)

        zero = jnp.zeros((8, LANES), jnp.float32)
        sums = lax.fori_loop(0, rows // chunk, body, (zero,) * (SLAB // LANES))
        for i in range(SLAB // LANES):
            parts[2 * j + p, me, :, pl.ds(i * LANES, LANES)] = sums[i]

    def share_sums(j, p):
        for k in range(1, n):
            part_copy(j, p, k, me).start()

    def finish(j, p):
        t = 2 * j + p
        for k in range(1, n):
            part_copy(j, p, k, lax.rem(me + n - k, n)).wait_recv()
        total = parts[t, 0]
        for r in range(1, n):
            total = total + parts[t, r]
        column = jnp.sum(total, axis=0, keepdims=True) / (n * rows)
        cols[p][:, columns(j)] = column
        factor = 1.0 / column

        def body(c, carry):
            at = pl.ds(pl.multiple_of(c * chunk, chunk), chunk)
            to = pl.ds(pl.multiple_of(me * rows + c * chunk, chunk), chunk)
            outs[p][to, columns(j)] = (held[p, at, :] * factor).astype(jnp.bfloat16)
            return carry

        lax.fori_loop(0, rows // chunk, body, 0)

    def share_rows(j, p):
        for k in range(1, n):
            row_copy(j, p, k, me).start()

    gain_copy = pltpu.make_async_copy(gain, gain_buf, gain_sem)
    gain_copy.start()
    ahead = min(SLOTS // 2, slabs)
    for j in range(ahead):
        for p in range(2):
            for copy in loads(j, p):
                copy.start()

    barrier = pltpu.get_barrier_semaphore()
    for k in range(1, n):
        pl.semaphore_signal(barrier, inc=1, device_id={"rows": lax.rem(me + k, n)}, device_id_type=MESH)

    gain_copy.wait()
    for r in range(rows // LANES):
        spread = jnp.broadcast_to(gain_buf[r : r + 1, :], (LANES, LANES)).T
        at = pl.ds(r * LANES, LANES)
        keep_scale[at, :] = spread * (1.0 - learn_rate * decay_rate)
        step_scale[at, :] = spread * learn_rate

    pl.semaphore_wait(barrier, n - 1)

    def refill(j, p):
        @pl.when(j + ahead < slabs)
        def _():
            for copy in loads(j + ahead, p):
                copy.start()

    def step(j, carry):
        update(j, 0)
        share_sums(j, 0)
        refill(j, 0)

        @pl.when(j > 0)
        def _():
            finish(j - 1, 1)
            share_rows(j - 1, 1)

        update(j, 1)
        share_sums(j, 1)
        refill(j, 1)
        finish(j, 0)
        share_rows(j, 0)
        return carry

    lax.fori_loop(0, slabs, step, 0)
    finish(slabs - 1, 1)
    share_rows(slabs - 1, 1)

    def drain(j, carry):
        for p in range(2):
            for k in range(1, n):
                part_copy(j, p, k, me).wait_send()
                row_copy(j, p, k, me).wait_send()
                row_copy(j, p, k, lax.rem(me + n - k, n)).wait_recv()
        return carry

    lax.fori_loop(0, slabs, drain, 0)


def store_kernel(pieces, gate, up, col_g, col_u, out_g, out_u, out_cg, out_cu, sem, col_sem):
    height = gate.shape[0] // pieces
    copies = []
    for p, (source, target) in enumerate(((gate, out_g), (up, out_u))):
        for i in range(pieces):
            at = pl.ds(i * height, height)
            copies.append(pltpu.make_async_copy(source.at[at, :], target.at[at, :], sem.at[p, i]))
    copies.append(pltpu.make_async_copy(col_g, out_cg, col_sem.at[0]))
    copies.append(pltpu.make_async_copy(col_u, out_cu, col_sem.at[1]))
    for copy in copies:
        copy.start()
    for copy in copies:
        copy.wait()


def solution(mesh):
    n = mesh.shape["rows"]

    def shards(weight_gate, moment_gate, square_gate, weight_up, moment_up, square_up, norm_gain):
        rows, width = weight_gate.shape
        steps = 2 * (width // SLAB)
        any_space = pl.BlockSpec(memory_space=pl.ANY)
        in_vmem = pl.BlockSpec(memory_space=pltpu.VMEM)
        shapes = (
            ((n * rows, width), jnp.bfloat16),
            ((n * rows, width), jnp.bfloat16),
            ((1, width), jnp.float32),
            ((1, width), jnp.float32),
        )
        dma = pltpu.SemaphoreType.DMA
        moved = pl.pallas_call(
            functools.partial(exchange_kernel, n),
            out_shape=tuple(pltpu.VMEM(*shape) for shape in shapes),
            in_specs=[any_space] * 7,
            out_specs=[in_vmem] * 4,
            scratch_shapes=[
                pltpu.VMEM((SLOTS, rows, SLAB), jnp.float32),
                pltpu.VMEM((SLOTS, rows, SLAB), jnp.float32),
                pltpu.VMEM((SLOTS, rows, SLAB), jnp.float32),
                pltpu.VMEM((2, rows, SLAB), jnp.float32),
                pltpu.VMEM((rows // LANES, LANES), jnp.float32),
                pltpu.VMEM((rows, LANES), jnp.float32),
                pltpu.VMEM((rows, LANES), jnp.float32),
                pltpu.VMEM((steps, n, 8, SLAB), jnp.float32),
                dma,
                dma((SLOTS, 3)),
                dma((steps, max(n - 1, 1))),
                dma((steps, max(n - 1, 1))),
                dma((steps, max(n - 1, 1))),
                dma((steps, max(n - 1, 1))),
            ],
            compiler_params=pltpu.CompilerParams(
                collective_id=0, has_side_effects=True, vmem_limit_bytes=36 * 1024 * 1024
            ),
            name="exchange",
        )(
            weight_gate, moment_gate, square_gate, weight_up, moment_up, square_up,
            norm_gain.reshape(rows // LANES, LANES),
        )
        pieces = 4
        gate, up, col_g, col_u = pl.pallas_call(
            functools.partial(store_kernel, pieces),
            out_shape=tuple(jax.ShapeDtypeStruct(*shape) for shape in shapes),
            in_specs=[in_vmem] * 4,
            out_specs=[any_space] * 4,
            scratch_shapes=[dma((2, pieces)), dma((2,))],
            compiler_params=pltpu.CompilerParams(vmem_limit_bytes=1024 * 1024),
            name="store",
        )(*moved)
        return gate, up, col_g.reshape(width), col_u.reshape(width)

    held = P(("trial", "rows"), "cols")
    return jax.shard_map(
        shards,
        mesh=mesh,
        in_specs=(held,) * 6 + (P(("trial", "rows")),),
        out_specs=(P("trial", "cols"), P("trial", "cols"), P(("trial", "cols")), P(("trial", "cols"))),
        check_vma=False,
    )
```
